256 devices in a mesh: seq: 64 (over z_hi, x, y), head: 4 (over z_lo, core).
Axes of the slice: x: 4, y: 4, z: 8 (z_hi: 4, z_lo: 2; z = z_hi * 2 + z_lo), core: 2. Of those that a mesh axis runs over, the one named last changes fastest.
Arguments:
- queries: bfloat16 [16384, 768], P('seq', 'head'), may hold values from -9 to 9
- keys: bfloat16 [16384, 768], P('seq', 'head'), may hold values from -12 to 12
- values: bfloat16 [16384, 768], P('seq', 'head'), may hold values from -6 to 6
- out_weight: bfloat16 [768, 1536], replicated, may hold values from -0.21875 to 0.21875
- out_grad: bfloat16 [16384, 1536], P('seq', 'head'), may hold values from -6 to 6
Outputs:
- projected: bfloat16 [16384, 1536], P('seq', 'head')
- query_grad: bfloat16 [16384, 768], P('seq', 'head')
- key_grad: bfloat16 [16384, 768], P('seq', 'head')
- value_grad: bfloat16 [16384, 768], P('seq', 'head')
The draws below stay inside these ranges and needn't reach their ends.
All inputs are finite; a program needn't handle non-finite values.
Results may differ from the reference program's by a relative error of at most 0.02.
Values may be sent and summed in bfloat16 or wider, within the bound.
No kernel may reach another device: no remote copies, remote signals or barrier semaphores. Data moves between devices by JAX's collectives and lax.ppermute only.
A program may use at most 128 MiB of HBM per device.

```python
import math
import jax
import jax.numpy as jnp
from jax import lax

D = 1536
HEADS = 12
HD = 64
NC = 16384


def draw_queries(key, part):
    base = jnp.clip(1.5 * jax.random.normal(jax.random.fold_in(key, 1), (NC, HEADS * HD), jnp.float32), -9.0, 9.0)
    return base.astype(jnp.bfloat16)


def draw_keys(key, part):
    base = jnp.clip(2.0 * jax.random.normal(jax.random.fold_in(key, 2), (NC, HEADS * HD), jnp.float32), -12.0, 12.0)
    return base.astype(jnp.bfloat16)


def level_of(rng, extent, pieces, least, high):
    def one(axis_at, blocks):
        steps = jax.random.uniform(jax.random.fold_in(jax.random.fold_in(rng, 6), axis_at), (blocks,), jnp.float32, least / len(pieces), high / len(pieces))
        return jnp.repeat(jnp.exp(steps), extent[axis_at] // blocks).reshape((-1,) + (1,) * (len(extent) - axis_at - 1))

    loudness = one(*pieces[0])
    for cut in pieces[1:]:
        loudness = loudness * one(*cut)
    return loudness


def gaussian(key, extent, deviation, bound, pieces=(), kind=jnp.bfloat16):
    entries = deviation * jax.random.normal(key, extent, jnp.float32)
    if pieces:
        entries = entries * level_of(key, extent, pieces, -0.22, 0.18)
    return jnp.clip(entries, -bound, bound).astype(kind)


def setup_inputs(seed: int = 0) -> dict:
    splits = jax.random.split(jax.random.key(seed), 6)
    queries = draw_queries(jax.random.fold_in(splits[5], 71), 0)
    keys = draw_keys(jax.random.fold_in(splits[5], 71), 0)
    values = gaussian(splits[2], (NC, HEADS * HD), 1.0, 6.0, ((0, 64), (1, 4)))
    out_weight = gaussian(splits[3], (HEADS * HD, D), (HEADS * HD) ** -0.5, 0.21875)
    out_grad = gaussian(splits[4], (NC, D), 1.0, 6.0, ((0, 64), (1, 4)))
    return dict(queries=queries, keys=keys, values=values, out_weight=out_weight, out_grad=out_grad)


masked_score = -1e30


def head_forward(query_head, key_head, value_head):
    count_rows = query_head.shape[0]
    block_rows = math.gcd(512, count_rows)
    key_pos = jnp.arange(count_rows, dtype=jnp.int32)
    score_scale = HD ** -0.5

    def query_block(block_index):
        first_row = block_index * block_rows
        query_part = lax.dynamic_slice_in_dim(query_head, first_row, block_rows, 0)
        scores = jnp.dot(query_part, key_head.T, preferred_element_type=jnp.float32) * score_scale
        query_pos = first_row + jnp.arange(block_rows, dtype=jnp.int32)
        causal = key_pos[None, :] <= query_pos[:, None]
        scores = jnp.where(causal, scores, masked_score)
        row_max = jnp.max(scores, axis=1, keepdims=True)
        weights = jnp.where(causal, jnp.exp(scores - row_max), 0.0)
        denominator = jnp.sum(weights, axis=1, keepdims=True)
        mixed = jnp.dot(weights.astype(jnp.bfloat16), value_head, preferred_element_type=jnp.float32) / denominator
        return mixed.astype(jnp.bfloat16), (row_max + jnp.log(denominator))[:, 0]

    outputs, log_total = lax.map(query_block, jnp.arange(count_rows // block_rows, dtype=jnp.int32))
    return outputs.reshape(count_rows, HD), log_total.reshape(count_rows)


def head_backward(query_head, key_head, value_head, grad_head, log_total, row_dot):
    count_rows = query_head.shape[0]
    block_rows = math.gcd(512, count_rows)
    all_pos = jnp.arange(count_rows, dtype=jnp.int32)
    score_scale = HD ** -0.5

    def query_block(block_index):
        first_row = block_index * block_rows
        query_part = lax.dynamic_slice_in_dim(query_head, first_row, block_rows, 0)
        grad_part = lax.dynamic_slice_in_dim(grad_head, first_row, block_rows, 0)
        log_part = lax.dynamic_slice_in_dim(log_total, first_row, block_rows, 0)
        dot_part = lax.dynamic_slice_in_dim(row_dot, first_row, block_rows, 0)
        query_pos = first_row + jnp.arange(block_rows, dtype=jnp.int32)
        causal = all_pos[None, :] <= query_pos[:, None]
        scores = jnp.dot(query_part, key_head.T, preferred_element_type=jnp.float32) * score_scale
        scores = jnp.where(causal, scores, masked_score)
        probability = jnp.exp(scores - log_part[:, None])
        prob_grad = jnp.dot(grad_part, value_head.T, preferred_element_type=jnp.float32)
        dscore = probability * (prob_grad - dot_part[:, None])
        result = jnp.dot(dscore.astype(jnp.bfloat16), key_head, preferred_element_type=jnp.float32) * score_scale
        return result.astype(jnp.bfloat16)

    def key_block(block_index):
        first_row = block_index * block_rows
        key_part = lax.dynamic_slice_in_dim(key_head, first_row, block_rows, 0)
        value_part = lax.dynamic_slice_in_dim(value_head, first_row, block_rows, 0)
        key_pos = first_row + jnp.arange(block_rows, dtype=jnp.int32)
        causal = key_pos[None, :] <= all_pos[:, None]
        scores = jnp.dot(query_head, key_part.T, preferred_element_type=jnp.float32) * score_scale
        scores = jnp.where(causal, scores, masked_score)
        probability = jnp.exp(scores - log_total[:, None])
        value_result = jnp.dot(probability.astype(jnp.bfloat16).T, grad_head, preferred_element_type=jnp.float32)
        prob_grad = jnp.dot(grad_head, value_part.T, preferred_element_type=jnp.float32)
        dscore = probability * (prob_grad - row_dot[:, None])
        key_result = jnp.dot(dscore.astype(jnp.bfloat16).T, query_head, preferred_element_type=jnp.float32) * score_scale
        return key_result.astype(jnp.bfloat16), value_result.astype(jnp.bfloat16)

    block_ids = jnp.arange(count_rows // block_rows, dtype=jnp.int32)
    query_result = lax.map(query_block, block_ids).reshape(count_rows, HD)
    key_result, value_result = lax.map(key_block, block_ids)
    return query_result, key_result.reshape(count_rows, HD), value_result.reshape(count_rows, HD)


def reference(queries, keys, values, out_weight, out_grad):
    count_rows = queries.shape[0]

    def by_head(matrix):
        return matrix.reshape(count_rows, HEADS, HD).transpose(1, 0, 2)

    def merge_heads(stacked):
        return stacked.transpose(1, 0, 2).reshape(count_rows, HEADS * HD)

    def forward_one(triple):
        return head_forward(triple[0], triple[1], triple[2])

    query_heads, key_heads, value_heads = by_head(queries), by_head(keys), by_head(values)
    attended_heads, log_total = lax.map(forward_one, (query_heads, key_heads, value_heads))
    attended = merge_heads(attended_heads)
    projected = jnp.dot(attended, out_weight, preferred_element_type=jnp.float32).astype(jnp.bfloat16)
    output_grad = lax.dot_general(out_grad, out_weight, (((1,), (1,)), ((), ())), preferred_element_type=jnp.float32).astype(jnp.bfloat16)
    row_dot = jnp.sum((output_grad.astype(jnp.float32) * attended.astype(jnp.float32)).reshape(count_rows, HEADS, HD), axis=2).T

    def backward_one(group_args):
        return head_backward(group_args[0], group_args[1], group_args[2], group_args[3], group_args[4], group_args[5])

    query_result, key_result, value_result = lax.map(backward_one, (query_heads, key_heads, value_heads, by_head(output_grad), log_total, row_dot))
    return projected, merge_heads(query_result), merge_heads(key_result), merge_heads(value_result)
```

```python
import math

import jax
import jax.numpy as jnp
from jax import lax
from jax.experimental import pallas as pl
from jax.experimental.pallas import tpu as pltpu
from jax.sharding import Mesh, PartitionSpec as P

HD = 64
HEADS_HERE = 3
WIDTH = HEADS_HERE * HD
HALF = 128
C2 = HD**-0.5 * math.log2(math.e)
LOW = -1e30
NT = (((1,), (1,)), ((), ()))
NN = (((1,), (0,)), ((), ()))


def dot(a, b, dims):
    return lax.dot_general(a, b, dims, preferred_element_type=jnp.float32)


def chunk_of(ref, n, a, h):
    pair = ref[pl.ds(n, 2), :, a * WIDTH + h * HD : a * WIDTH + (h + 1) * HD]
    return pair.reshape(2 * HALF, HD)


def column_of(place):
    return place[1] * 4 + place[2]


def causal_mask(place, n, a):
    c = column_of(place)
    k = lax.broadcasted_iota(jnp.int32, (2 * HALF, 2 * HALF), 0)
    q = lax.broadcasted_iota(jnp.int32, (2 * HALF, 2 * HALF), 1)
    k_pos = jnp.where(k < HALF, c * 256 + k, (15 - c) * 256 + k)
    q_pos = n * 256 + a * HALF + jnp.where(q < HALF, q, q + HALF)
    return k_pos <= q_pos


def has_diagonal(place, n):
    c = column_of(place)
    return jnp.where(n + 1 >= jnp.minimum(c, 15 - c), 1, 0)


def stage_rows(place, refs, out, outer_is_x):
    for i in range(4):
        for j in range(4):
            kx, ky = (i, j) if outer_is_x else (j, i)
            n = ((place[1] - kx) & 3) * 4 + ((place[2] - ky) & 3)
            out[n] = refs[i][j]


def forward_kernel(place, *refs):
    q_refs, kv_refs = refs[:4], refs[4:12]
    o_ref, lse_ref, q_ref, k_s, v_s = refs[12:]
    stage_rows(place, q_refs, q_ref, False)
    for slot in range(4):
        z = (place[0] - slot) & 3
        kv = jnp.concatenate([kv_refs[slot][...], kv_refs[4 + slot][...]], axis=0)
        for h in range(HEADS_HERE):
            k_s[h, z] = kv[:, h * HD : (h + 1) * HD]
            v_t = kv[:, WIDTH + h * HD : WIDTH + (h + 1) * HD].astype(jnp.float32).T
            v_s[h, z] = jnp.concatenate([v_t, jnp.ones_like(v_t)], axis=0).astype(jnp.bfloat16)
    for a in range(2):
        zq = place[0] if a == 0 else 3 - place[0]

        def chunk(t, _):
            n = 2 * t
            queries = [chunk_of(q_ref, n, a, h) for h in range(HEADS_HERE)]

            def step(z, state, mask=None):
                new = []
                for h in range(HEADS_HERE):
                    m, acc = state[h]
                    s = dot(k_s[h, z], queries[h], NT) * C2
                    if mask is not None:
                        s = jnp.where(mask, s, LOW)
                    m_new = jnp.maximum(m, jnp.max(s, axis=0, keepdims=True))
                    p = jnp.exp2(s - m_new)
                    if mask is not None:
                        p = jnp.where(mask, p, 0.0)
                    acc = acc * jnp.exp2(m - m_new) + dot(v_s[h, z], p.astype(jnp.bfloat16), NN)
                    new.append((m_new, acc))
                return tuple(new)

            state = tuple(
                (jnp.full((1, 2 * HALF), LOW, jnp.float32), jnp.zeros((2 * HD, 2 * HALF), jnp.float32))
                for _ in range(HEADS_HERE)
            )
            state = lax.fori_loop(0, zq, step, state)
            state = lax.fori_loop(
                0, has_diagonal(place, n), lambda i, st: step(zq, st, causal_mask(place, n, a)), state
            )
            for h in range(HEADS_HERE):
                m, acc = state[h]
                total = acc[HD : HD + 1]
                some = total > 0.0
                safe = jnp.where(some, total, 1.0)
                o = (acc[:HD] * (1.0 / safe)).astype(jnp.bfloat16)
                lse = jnp.where(some, m + jnp.log2(safe), LOW)
                for i in range(2):
                    row = a * WIDTH + h * HD
                    o_ref[n + i, row : row + HD, :] = o[:, i * HALF : (i + 1) * HALF]
                    lse_ref[n + i, a * HEADS_HERE + h, :] = lse[0, i * HALF : (i + 1) * HALF]
            return 0

        lax.fori_loop(0, 8, chunk, 0)


def backward_kernel(place, *refs):
    q_refs, g_refs, kv_refs, stat_ref = refs[:4], refs[4:8], refs[8:16], refs[16]
    dq_ref, dkv_ref, q_ref, g_ref, k_s, kt_s, v_s, dk_s, dv_s = refs[17:]
    stage_rows(place, q_refs, q_ref, False)
    stage_rows(place, g_refs, g_ref, True)
    for slot in range(4):
        z = (place[0] - slot) & 3
        kv = jnp.concatenate([kv_refs[slot][...], kv_refs[4 + slot][...]], axis=0)
        for h in range(HEADS_HERE):
            k = kv[:, h * HD : (h + 1) * HD]
            k_s[h, z] = k
            kt_s[h, z] = k.astype(jnp.float32).T.astype(jnp.bfloat16)
            v_s[h, z] = kv[:, WIDTH + h * HD : WIDTH + (h + 1) * HD]
    dk_s[...] = jnp.zeros_like(dk_s)
    dv_s[...] = jnp.zeros_like(dv_s)
    for a in range(2):
        zq = place[0] if a == 0 else 3 - place[0]

        def chunk(t, _):
            n = 2 * t
            queries = [chunk_of(q_ref, n, a, h) for h in range(HEADS_HERE)]
            grads = [chunk_of(g_ref, n, a, h) for h in range(HEADS_HERE)]

            def row_of(j):
                return jnp.concatenate([stat_ref[n, j : j + 1, :], stat_ref[n + 1, j : j + 1, :]], axis=1)

            logs = [row_of(a * HEADS_HERE + h) for h in range(HEADS_HERE)]
            dots = [row_of(8 + a * HEADS_HERE + h) for h in range(HEADS_HERE)]

            def step(z, state, mask=None):
                new = []
                for h in range(HEADS_HERE):
                    s = dot(k_s[h, z], queries[h], NT) * C2
                    p = jnp.exp2(s - logs[h])
                    if mask is not None:
                        p = jnp.where(mask, p, 0.0)
                    dv_s[h, z] += dot(p.astype(jnp.bfloat16), grads[h], NN)
                    dp = dot(v_s[h, z], grads[h], NT)
                    ds = (p * (dp - dots[h])).astype(jnp.bfloat16)
                    dk_s[h, z] += dot(ds, queries[h], NN)
                    new.append(state[h] + dot(kt_s[h, z], ds, NN))
                return tuple(new)

            state = tuple(jnp.zeros((HD, 2 * HALF), jnp.float32) for _ in range(HEADS_HERE))
            state = lax.fori_loop(0, zq, step, state)
            state = lax.fori_loop(
                0, has_diagonal(place, n), lambda i, st: step(zq, st, causal_mask(place, n, a)), state
            )
            for h in range(HEADS_HERE):
                dq = (state[h] * HD**-0.5).astype(jnp.bfloat16)
                for i in range(2):
                    row = a * WIDTH + h * HD
                    dq_ref[n + i, row : row + HD, :] = dq[:, i * HALF : (i + 1) * HALF]
            return 0

        lax.fori_loop(0, 8, chunk, 0)
    for slot in range(4):
        z = (place[0] - slot) & 3
        parts = [dk_s[h, z] * HD**-0.5 for h in range(HEADS_HERE)] + [dv_s[h, z] for h in range(HEADS_HERE)]
        dkv_ref[slot] = jnp.concatenate(parts, axis=1).astype(jnp.bfloat16).reshape(2, HALF, 2 * WIDTH)


SMEM = pl.BlockSpec(memory_space=pltpu.SMEM)
VMEM = pl.BlockSpec(memory_space=pltpu.VMEM)
ROWS = pltpu.VMEM((16, HALF, 2 * WIDTH), jnp.bfloat16)
KEYS = pltpu.VMEM((HEADS_HERE, 4, 2 * HALF, HD), jnp.bfloat16)
KEYS_T = pltpu.VMEM((HEADS_HERE, 4, HD, 2 * HALF), jnp.bfloat16)
SUMS = pltpu.VMEM((HEADS_HERE, 4, 2 * HALF, HD), jnp.float32)


def forward_tile(place, q, kv):
    return pl.pallas_call(
        forward_kernel,
        out_shape=(
            jax.ShapeDtypeStruct((16, 2 * WIDTH, HALF), jnp.bfloat16),
            jax.ShapeDtypeStruct((16, 8, HALF), jnp.float32),
        ),
        in_specs=[SMEM] + [VMEM] * 12,
        out_specs=(VMEM, VMEM),
        scratch_shapes=[ROWS, KEYS, pltpu.VMEM((HEADS_HERE, 4, 2 * HD, 2 * HALF), jnp.bfloat16)],
        name="forward_tile",
    )(place, *q, *kv)


def backward_tile(place, q, g, kv, stats):
    return pl.pallas_call(
        backward_kernel,
        out_shape=(
            jax.ShapeDtypeStruct((16, 2 * WIDTH, HALF), jnp.bfloat16),
            jax.ShapeDtypeStruct((4, 2, HALF, 2 * WIDTH), jnp.bfloat16),
        ),
        in_specs=[SMEM] + [VMEM] * 17,
        out_specs=(VMEM, VMEM),
        scratch_shapes=[ROWS, ROWS, KEYS, KEYS_T, KEYS, SUMS, SUMS],
        name="backward_tile",
    )(place, *q, *g, *kv, stats)


GRID = ("z", "x", "y")


def across_z(k, mirrored=False):
    pairs = []
    for z in range(4):
        for c in range(16):
            pairs.append((16 * z + c, 16 * ((z + k) % 4) + (15 - c if mirrored else c)))
    return pairs


def shifts(x, axis):
    moved = [lax.ppermute(x, axis, [(i, (i + k) % 4) for i in range(4)]) for k in (1, 2, 3)]
    return [x, *moved]


def swapped(x):
    return lax.ppermute(x, "z", [(i, 3 - i) for i in range(4)])


def zigzag(first, second):
    return jnp.concatenate([first, swapped(second)], axis=1)


def gathered(x, first_axis, second_axis):
    return shifts(jnp.stack(shifts(x, first_axis)), second_axis)


def to_owners(x):
    return lax.all_to_all(x, ("x", "y"), 0, 0, tiled=True)


def rows_of(first, second):
    return jnp.concatenate([first.T, second.T], axis=0)


def per_device(queries, keys, values, out_weight, out_grad):
    head = lax.axis_index("head")
    place = jnp.stack([lax.axis_index(a) for a in GRID]).astype(jnp.int32)
    cols = out_grad.shape[1]
    own_cols = lax.dynamic_slice_in_dim(out_weight, head * cols, cols, 1)

    def weight_rows(group):
        return lax.dynamic_slice_in_dim(own_cols, group * WIDTH, WIDTH, 0)

    halves = [
        jnp.concatenate([keys[b * HALF : (b + 1) * HALF], values[b * HALF : (b + 1) * HALF]], axis=1)
        for b in range(2)
    ]
    q_all = gathered(zigzag(queries[:HALF], queries[HALF:]), "x", "y")
    kv_all = [halves[0]] + [lax.ppermute(halves[0], GRID, across_z(k)) for k in (1, 2, 3)]
    kv_all += [lax.ppermute(halves[1], GRID, across_z(k, True)) for k in range(4)]

    grad_parts = []
    for k in range(4):
        part = dot(out_grad, weight_rows((head + k) & 3), NT)
        part = jnp.concatenate([part[:HALF], part[HALF:]], axis=1)
        if k:
            part = part.astype(jnp.bfloat16)
            part = lax.ppermute(part, "head", [(i, (i + k) % 4) for i in range(4)])
        grad_parts.append(part.astype(jnp.float32))
    grads = sum(grad_parts).astype(jnp.bfloat16)
    g_own = zigzag(grads[:, :WIDTH], grads[:, WIDTH:])
    g_all = gathered(g_own, "y", "x")

    o_part, lse_part = forward_tile(place, q_all, kv_all)
    o_part, lse_part = to_owners(o_part), to_owners(lse_part)
    top = jnp.max(lse_part, axis=0)
    share = jnp.exp2(lse_part - top)
    total = jnp.sum(share, axis=0)
    lse = top + jnp.log2(total)
    share = (share / total)[:, :6]
    mixed = jnp.sum(
        o_part.reshape(16, 6, HD, HALF).astype(jnp.float32) * share[:, :, None, :], axis=0
    )
    mixed = mixed.astype(jnp.bfloat16)
    row_dot = jnp.sum(
        mixed.astype(jnp.float32) * g_own.T.reshape(6, HD, HALF).astype(jnp.float32), axis=1
    )
    stats = jnp.concatenate([lse, jnp.pad(row_dot, ((0, 2), (0, 0)))], axis=0)
    stats = to_owners(jnp.broadcast_to(stats, (16, *stats.shape)))

    dq_part, dkv_part = backward_tile(place, q_all, g_all, kv_all, stats)

    mixed = mixed.reshape(2 * WIDTH, HALF)
    attended = jnp.concatenate([mixed[:WIDTH], swapped(mixed[WIDTH:])], axis=1)
    projected = sum(
        lax.dot_general(
            part, weight_rows((head - k) & 3), (((0,), (0,)), ((), ())), preferred_element_type=jnp.float32
        )
        for k, part in enumerate(shifts(attended, "head"))
    ).astype(jnp.bfloat16)

    dq = jnp.sum(to_owners(dq_part).astype(jnp.float32), axis=0).astype(jnp.bfloat16)
    query_grad = rows_of(dq[:WIDTH], swapped(dq[WIDTH:]))
    own = []
    for b in range(2):
        total = None
        for k in range(4):
            part = dkv_part[k, b]
            if k or b:
                part = lax.ppermute(part, GRID, across_z(-k, b == 1))
            part = part.astype(jnp.float32)
            total = part if total is None else total + part
        own.append(total.astype(jnp.bfloat16))
    own = jnp.concatenate(own, axis=0)
    return projected, query_grad, own[:, :WIDTH], own[:, WIDTH:]


def solution(mesh):
    grid = Mesh(mesh.devices.reshape(4, 4, 4, 4), ("z", "x", "y", "head"))
    split = P(GRID, "head")
    return jax.shard_map(
        per_device,
        mesh=grid,
        in_specs=(split, split, split, P(), split),
        out_specs=(split, split, split, split),
        check_vma=False,
    )
```

```python
import math

import jax
import jax.numpy as jnp
from jax import lax
from jax.experimental import pallas as pl
from jax.experimental.pallas import tpu as pltpu
from jax.sharding import PartitionSpec as P


HD = 64
HEADS_HERE = 3
WIDTH = HEADS_HERE * HD
HALF = 128
TILE = 2 * HALF
C2 = HD**-0.5 * math.log2(math.e)
LOW = -1e30
NT = (((1,), (1,)), ((), ()))
NN = (((1,), (0,)), ((), ()))
TN = (((0,), (0,)), ((), ()))
HERE = range(HEADS_HERE)


def dot(a, b, dims=NN):
    return lax.dot_general(a, b, dims, preferred_element_type=jnp.float32)


def pair_of(ref, n, row, rows):
    return jnp.concatenate([ref[n, row : row + rows, :], ref[n + 1, row : row + rows, :]], axis=1)


def causal_mask(place, n, a):
    c = place[1]
    k = lax.broadcasted_iota(jnp.int32, (TILE, TILE), 0)
    q = lax.broadcasted_iota(jnp.int32, (TILE, TILE), 1)
    k_pos = jnp.where(k < HALF, c * TILE + k, (15 - c) * TILE + k)
    q_pos = n * TILE + a * HALF + jnp.where(q < HALF, q, q + HALF)
    return k_pos <= q_pos


def has_diagonal(place, n):
    c = place[1]
    return jnp.where(n + 1 >= jnp.minimum(c, 15 - c), 1, 0)


def slot_rows(place, kv_refs):
    for slot in range(4):
        yield (place[0] - slot) & 3, kv_refs[slot][...].reshape(TILE, 2 * WIDTH)


def forward_kernel(place, q_ref, *refs):
    kv_refs, (o_ref, lse_ref, k_s, v_s) = refs[:4], refs[4:]
    for z, kv in slot_rows(place, kv_refs):
        for h in HERE:
            k_s[h, z] = kv[:, h * HD : (h + 1) * HD]
            v_t = kv[:, WIDTH + h * HD : WIDTH + (h + 1) * HD].astype(jnp.float32).T
            v_s[h, z] = jnp.concatenate([v_t, jnp.ones_like(v_t)], axis=0).astype(jnp.bfloat16)
    lse_ref[...] = jnp.zeros_like(lse_ref)
    for a in range(2):
        zq = place[0] if a == 0 else 3 - place[0]

        def chunk(t, _):
            n = 2 * t
            queries = [pair_of(q_ref, n, a * WIDTH + h * HD, HD) for h in HERE]

            def step(z, state, mask=None):
                s = [dot(k_s[h, z], queries[h]) * C2 for h in HERE]
                if mask is not None:
                    s = [jnp.where(mask, x, LOW) for x in s]
                top = [jnp.maximum(state[h][0], jnp.max(s[h], axis=0, keepdims=True)) for h in HERE]
                p = [jnp.exp2(s[h] - top[h]) for h in HERE]
                if mask is not None:
                    p = [jnp.where(mask, x, 0.0) for x in p]
                p = [x.astype(jnp.bfloat16) for x in p]
                add = [dot(v_s[h, z], p[h]) for h in HERE]
                return tuple(
                    (top[h], state[h][1] * jnp.exp2(state[h][0] - top[h]) + add[h]) for h in HERE
                )

            state = tuple(
                (jnp.full((1, TILE), LOW, jnp.float32), jnp.zeros((2 * HD, TILE), jnp.float32))
                for _ in HERE
            )
            state = lax.fori_loop(0, zq, step, state)
            state = lax.fori_loop(
                0, has_diagonal(place, n), lambda i, st: step(zq, st, causal_mask(place, n, a)), state
            )
            for h in HERE:
                top, acc = state[h]
                total = acc[HD : HD + 1]
                some = total > 0.0
                safe = jnp.where(some, total, 1.0)
                o = (acc[:HD] * (1.0 / safe)).astype(jnp.bfloat16)
                lse = jnp.where(some, top + jnp.log2(safe), LOW)
                for i in range(2):
                    row = a * WIDTH + h * HD
                    o_ref[n + i, row : row + HD, :] = o[:, i * HALF : (i + 1) * HALF]
                    lse_ref[n + i, a * HEADS_HERE + h, :] = lse[0, i * HALF : (i + 1) * HALF]
            return 0

        lax.fori_loop(0, 8, chunk, 0)


def row_dot_kernel(o_ref, g_ref, lse_ref, out_ref):
    def block(n, _):
        product = o_ref[n].astype(jnp.float32) * g_ref[n].astype(jnp.float32)
        sums = [jnp.sum(product[j * HD : (j + 1) * HD], axis=0, keepdims=True) for j in range(6)]
        out_ref[n, :8, :] = lse_ref[n]
        out_ref[n, 8:, :] = jnp.concatenate(sums + [jnp.zeros((2, HALF), jnp.float32)], axis=0)
        return 0

    lax.fori_loop(0, 16, block, 0)


def backward_kernel(place, q_ref, g_ref, stat_ref, *refs):
    kv_refs, dq_ref, dkv_refs = refs[:4], refs[4], refs[5:9]
    k_s, kt_s, v_s, dk_s, dv_s = refs[9:]
    for z, kv in slot_rows(place, kv_refs):
        for h in HERE:
            k = kv[:, h * HD : (h + 1) * HD]
            k_s[h, z] = k
            kt_s[h, z] = k.astype(jnp.float32).T.astype(jnp.bfloat16)
            v_s[h, z] = kv[:, WIDTH + h * HD : WIDTH + (h + 1) * HD]
    dk_s[...] = jnp.zeros_like(dk_s)
    dv_s[...] = jnp.zeros_like(dv_s)
    for a in range(2):
        zq = place[0] if a == 0 else 3 - place[0]

        def chunk(t, _):
            n = 2 * t
            queries = [pair_of(q_ref, n, a * WIDTH + h * HD, HD) for h in HERE]
            grads = [pair_of(g_ref, n, a * WIDTH + h * HD, HD) for h in HERE]
            logs = [pair_of(stat_ref, n, a * HEADS_HERE + h, 1) for h in HERE]
            dots = [pair_of(stat_ref, n, 8 + a * HEADS_HERE + h, 1) for h in HERE]

            def step(z, state, mask=None):
                s = [dot(k_s[h, z], queries[h]) for h in HERE]
                dp = [dot(v_s[h, z], grads[h]) for h in HERE]
                p = [jnp.exp2(s[h] * C2 - logs[h]) for h in HERE]
                if mask is not None:
                    p = [jnp.where(mask, x, 0.0) for x in p]
                ds = [(p[h] * (dp[h] - dots[h])).astype(jnp.bfloat16) for h in HERE]
                for h in HERE:
                    dv_s[h, z] += dot(p[h].astype(jnp.bfloat16), grads[h], NT)
                    dk_s[h, z] += dot(ds[h], queries[h], NT)
                return tuple(state[h] + dot(kt_s[h, z], ds[h]) for h in HERE)

            state = tuple(jnp.zeros((HD, TILE), jnp.float32) for _ in HERE)
            state = lax.fori_loop(0, zq, step, state)
            state = lax.fori_loop(
                0, has_diagonal(place, n), lambda i, st: step(zq, st, causal_mask(place, n, a)), state
            )
            for h in HERE:
                dq = (state[h] * HD**-0.5).astype(jnp.bfloat16)
                for i in range(2):
                    row = a * WIDTH + h * HD
                    dq_ref[n + i, row : row + HD, :] = dq[:, i * HALF : (i + 1) * HALF]
            return 0

        lax.fori_loop(0, 8, chunk, 0)
    for slot in range(4):
        z = (place[0] - slot) & 3
        parts = [dk_s[h, z] * HD**-0.5 for h in HERE] + [dv_s[h, z] for h in HERE]
        both = jnp.concatenate(parts, axis=1).astype(jnp.bfloat16)
        dkv_refs[slot][...] = both.reshape(2, HALF, 2 * WIDTH)


SMEM = pl.BlockSpec(memory_space=pltpu.SMEM)
VMEM = pl.BlockSpec(memory_space=pltpu.VMEM)
KEYS = pltpu.VMEM((HEADS_HERE, 4, TILE, HD), jnp.bfloat16)
KEYS_T = pltpu.VMEM((HEADS_HERE, 4, HD, TILE), jnp.bfloat16)
SUMS = pltpu.VMEM((HEADS_HERE, 4, TILE, HD), jnp.float32)
ROWS = jax.ShapeDtypeStruct((16, 2 * WIDTH, HALF), jnp.bfloat16)


def forward_tile(place, q, kv):
    return pl.pallas_call(
        forward_kernel,
        out_shape=(ROWS, jax.ShapeDtypeStruct((16, 8, HALF), jnp.float32)),
        in_specs=[SMEM] + [VMEM] * 5,
        out_specs=(VMEM, VMEM),
        scratch_shapes=[KEYS, pltpu.VMEM((HEADS_HERE, 4, 2 * HD, TILE), jnp.bfloat16)],
        cost_estimate=pl.CostEstimate(flops=10**10, transcendentals=10**7, bytes_accessed=10**7),
        name="forward_tile",
    )(place, q, *kv)


def row_dot_tile(o, g, lse):
    return pl.pallas_call(
        row_dot_kernel,
        out_shape=jax.ShapeDtypeStruct((16, 16, HALF), jnp.float32),
        in_specs=[VMEM, VMEM, VMEM],
        out_specs=VMEM,
        name="row_dot_tile",
    )(o, g, lse)


def backward_tile(place, q, g, kv, stats):
    return pl.pallas_call(
        backward_kernel,
        out_shape=(ROWS,) + (jax.ShapeDtypeStruct((2, HALF, 2 * WIDTH), jnp.bfloat16),) * 4,
        in_specs=[SMEM] + [VMEM] * 7,
        out_specs=(VMEM,) * 5,
        scratch_shapes=[KEYS, KEYS_T, KEYS, SUMS, SUMS],
        cost_estimate=pl.CostEstimate(flops=2 * 10**10, transcendentals=10**7, bytes_accessed=10**7),
        name="backward_tile",
    )(place, q, g, stats, *kv)


PLANES = [[16 * z + c for c in range(16)] for z in range(4)]


def sent(x, to):
    pairs = []
    for z in range(4):
        for c in range(16):
            to_z, to_c = to(z, c)
            pairs.append((16 * z + c, 16 * (to_z % 4) + to_c))
    return lax.ppermute(x, "seq", pairs)


def swapped(x):
    return sent(x, lambda z, c: (3 - z, c))


def mirrored(x):
    return sent(x, lambda z, c: (z, 15 - c))


def to_head(x, k):
    return lax.ppermute(x, "head", [(i, (i + k) % 4) for i in range(4)])


def exchanged(x):
    return lax.all_to_all(x, "seq", 0, 0, axis_index_groups=PLANES, tiled=True)


def gathered(x):
    return exchanged(jnp.broadcast_to(x, (16, *x.shape)))


def whole(queries, keys, values, out_weight, out_grad):
    head = lax.axis_index("head")
    seat = lax.axis_index("seq")
    place = jnp.stack([seat // 16, seat % 16]).astype(jnp.int32)
    cols = out_grad.shape[1]
    own_cols = lax.dynamic_slice_in_dim(out_weight, head * cols, cols, 1)

    def weight_rows(group):
        return lax.dynamic_slice_in_dim(own_cols, (group & 3) * WIDTH, WIDTH, 0)

    moved = swapped(jnp.concatenate([queries[HALF:], out_grad[HALF:]], axis=1))
    halves = jnp.concatenate(
        [keys.reshape(2, HALF, WIDTH), values.reshape(2, HALF, WIDTH)], axis=2
    )
    second = mirrored(halves[1])
    q_own = jnp.concatenate([queries[:HALF].T, moved[:, :WIDTH].T], axis=0)
    q = gathered(q_own)
    own_kv = jnp.stack([halves[0], second])
    kv = [own_kv]
    for k in (1, 2, 3):
        kv.append(sent(own_kv, lambda z, c: (z + k, c)))

    grads = None
    grad_rows = (out_grad[:HALF], moved[:, WIDTH:])
    for k in (1, 2, 3, 0):
        part = jnp.concatenate([dot(weight_rows(head + k), x, NT) for x in grad_rows], axis=0)
        if k:
            part = to_head(part.astype(jnp.bfloat16), k).astype(jnp.float32)
        grads = part if grads is None else grads + part
    g = gathered(grads.astype(jnp.bfloat16))

    o_part, lse_part = forward_tile(place, q, kv)
    stats = row_dot_tile(o_part, g, lse_part)
    stats = exchanged(stats)
    o_part = exchanged(o_part)
    lse_part, dot_part = stats[:, :8], stats[:, 8:]
    top = jnp.max(lse_part, axis=0)
    share = jnp.exp2(lse_part - top)
    total = jnp.sum(share, axis=0)
    share = share / total
    row_dot = jnp.sum(share * dot_part, axis=0)
    stats = gathered(jnp.concatenate([top + jnp.log2(total), row_dot], axis=0))

    dq_part, *dkv_part = backward_tile(place, q, g, kv, stats)
    dq_part = exchanged(dq_part)

    own = dkv_part[0].astype(jnp.float32)
    for k in (1, 2, 3):
        own = own + sent(dkv_part[k], lambda z, c: (z - k, c)).astype(jnp.float32)
    own = own.astype(jnp.bfloat16)
    own = jnp.concatenate([own[0], mirrored(own[1])], axis=0)

    mixed = jnp.sum(
        o_part.reshape(16, 6, HD, HALF).astype(jnp.float32) * share[:, :6, None, :], axis=0
    )
    mixed = mixed.astype(jnp.bfloat16).reshape(2 * WIDTH, HALF)
    projected = [0.0, 0.0]
    for k in (1, 2, 3, 0):
        part = mixed
        if k:
            part = to_head(mixed, k)
        rows = weight_rows(head - k)
        for a in range(2):
            projected[a] = projected[a] + dot(part[a * WIDTH : (a + 1) * WIDTH], rows, TN)
    projected = [x.astype(jnp.bfloat16) for x in projected]

    dq = jnp.sum(dq_part.astype(jnp.float32), axis=0).astype(jnp.bfloat16)
    moved = swapped(jnp.concatenate([projected[1], dq[WIDTH:].T], axis=1))
    projected = jnp.concatenate([projected[0], moved[:, :cols]], axis=0)
    query_grad = jnp.concatenate([dq[:WIDTH].T, moved[:, cols:]], axis=0)
    return projected, query_grad, own[:, :WIDTH], own[:, WIDTH:]


def solution(mesh):
    split = P("seq", "head")
    return jax.shard_map(
        whole,
        mesh=mesh,
        in_specs=(split, split, split, P(), split),
        out_specs=(split, split, split, split),
        check_vma=False,
    )
```
